32 devices in a mesh: rep: 1, r: 4 (over z), s: 8 (over x, y, core).
Axes of the slice: x: 2, y: 2, z: 4, core: 2. Of those that a mesh axis runs over, the one named last changes fastest.
Arguments:
- x: bfloat16 [32, 4096, 640], P(('rep', 'r', 's'))
- dy: bfloat16 [32, 4096, 640], P(('rep', 'r', 's'))
- w_gate: bfloat16 [2, 640, 1792], P(None, 's')
- w_up: bfloat16 [2, 640, 1792], P(None, 's')
- w_down: bfloat16 [2, 1792, 640], P(None, 's')
- m_w_gate: float32 [2, 640, 1792], P(None, 's')
- m_w_up: float32 [2, 640, 1792], P(None, 's')
- m_w_down: float32 [2, 1792, 640], P(None, 's')
- v_w_gate: float32 [2, 640, 1792], P(None, 's')
- v_w_up: float32 [2, 640, 1792], P(None, 's')
- v_w_down: float32 [2, 1792, 640], P(None, 's')
Outputs:
- output 1: bfloat16 [2, 640, 1792], P('rep', 's')
- output 2: bfloat16 [2, 640, 1792], P('rep', 's')
- output 3: bfloat16 [2, 1792, 640], P('rep', 's')
- output 4: float32 [2, 640, 1792], P('rep', 's')
- output 5: float32 [2, 640, 1792], P('rep', 's')
- output 6: float32 [2, 1792, 640], P('rep', 's')
- output 7: float32 [2, 640, 1792], P('rep', 's')
- output 8: float32 [2, 640, 1792], P('rep', 's')
- output 9: float32 [2, 1792, 640], P('rep', 's')
All inputs are finite; a program needn't handle non-finite values.
Results may differ from the reference program's by a relative error of at most 0.02.
Values are sent between devices in bfloat16 or wider.
A program may use at most 2 GiB of HBM per device.

```python
import jax
import jax.numpy as jnp
from jax import lax

SEQUENCES = 32
TOKENS = 4096
D = 640
FF = 1792
LAYERS = 2
NAMES = ("w_gate", "w_up", "w_down")
SHAPES = {"w_gate": (LAYERS, D, FF), "w_up": (LAYERS, D, FF), "w_down": (LAYERS, FF, D)}


def bump(key, n, height):
    away = (jnp.arange(n, dtype=jnp.int32) - jax.random.randint(key, (), 0, n, jnp.int32)) % n
    return jnp.where(away < n // 8, height, 1.0)


def together(key, own, strength):
    shared = jax.random.normal(key, own.shape[1:], jnp.float32)
    return (own + strength * shared) * lax.rsqrt(1 + strength * strength)


def setup_inputs(seed: int = 0, part: int = 0) -> dict:
    kx, kdy, ka, kb, kz, kf, kh, kl, *keys = jax.random.split(jax.random.key(seed), 8 + 3 * len(NAMES))
    kx, kdy, ka, kb = (jax.random.fold_in(k, part) for k in (kx, kdy, ka, kb))
    kw, km, kv = (keys[i::3] for i in range(3))
    shape = (SEQUENCES, TOKENS, D)
    much_x, much_dy = jax.random.uniform(kz, (2,), jnp.float32, 0.0, 1.0)
    loud = 2.0 ** jax.random.uniform(jax.random.fold_in(kz, 1), (), jnp.float32, -1.0, 2.0)
    layers = 2.0 ** jax.random.uniform(kl, (LAYERS, 1, 1), jnp.float32, -1.0, 1.0)
    x = together(ka, jax.random.normal(kx, shape, jnp.float32), much_x) * bump(kf, D, 4.0)
    dy = together(kb, jax.random.normal(kdy, shape, jnp.float32), much_dy)
    drawn = {"x": x.astype(jnp.bfloat16), "dy": (loud * dy * (SEQUENCES * TOKENS) ** -0.5).astype(jnp.bfloat16)}
    for key, name in zip(kw, NAMES, strict=True):
        w = jax.random.normal(key, SHAPES[name], jnp.float32) * SHAPES[name][1] ** -0.5
        drawn[name] = (w * {"w_gate": 1.0, "w_up": bump(kh, FF, 4.0), "w_down": layers}[name]).astype(jnp.bfloat16)
    for key, name in zip(km, NAMES, strict=True):
        drawn[f"m_{name}"] = 0.1 * jax.random.normal(key, SHAPES[name], jnp.float32)
    for key, name in zip(kv, NAMES, strict=True):
        drawn[f"v_{name}"] = jax.random.uniform(key, SHAPES[name], jnp.float32, 0.005, 0.015)
    return drawn


def matmul(a, w):
    return jnp.dot(a, w, preferred_element_type=jnp.float32).astype(jnp.bfloat16)


def normed(h):
    wide = h.astype(jnp.float32)
    scale = lax.rsqrt(jnp.mean(wide**2, -1, keepdims=True) + 1e-6)
    return (wide * scale).astype(jnp.bfloat16)


def layer(h, w):
    a = normed(h)
    gate = jnp.dot(a, w["w_gate"], preferred_element_type=jnp.float32)
    up = jnp.dot(a, w["w_up"], preferred_element_type=jnp.float32)
    return h + matmul((jax.nn.silu(gate) * up).astype(jnp.bfloat16), w["w_down"])


def adamw(w, m, v, g):
    m = 0.9 * m + 0.1 * g
    v = 0.95 * v + 0.05 * g * g
    step = m * lax.rsqrt(v + 1e-8) + 0.1 * w
    return (w - 0.02 * step).astype(jnp.bfloat16), m, v


def stack(weights, h):
    return lax.scan(lambda h, w: (layer(h, w), None), h, weights)[0]


def reference(x, dy, w_gate, w_up, w_down, m_w_gate, m_w_up, m_w_down, v_w_gate, v_w_up, v_w_down):
    weights = dict(zip(NAMES, (w_gate, w_up, w_down), strict=True))

    def take(so_far, sequence):
        h, by_y = sequence
        _, back = jax.vjp(lambda w: stack(w, h), weights)
        return jax.tree.map(lambda total, term: total + term.astype(jnp.float32), so_far, back(by_y)[0]), None

    none_yet = {name: jnp.zeros(w.shape, jnp.float32) for name, w in weights.items()}
    by_weights, _ = lax.scan(take, none_yet, (x, dy))
    gradients = [by_weights[name].astype(jnp.bfloat16).astype(jnp.float32) for name in NAMES]
    new = [
        adamw(w.astype(jnp.float32), m, v, g)
        for w, m, v, g in zip((w_gate, w_up, w_down), (m_w_gate, m_w_up, m_w_down), (v_w_gate, v_w_up, v_w_down), gradients, strict=True)
    ]
    return tuple(one[which] for which in range(3) for one in new)
```

```python
import functools

import jax
import jax.numpy as jnp
from jax import lax
from jax.experimental import pallas as pl
from jax.experimental.pallas import tpu as pltpu
from jax.sharding import PartitionSpec as P

NAMES = ("w_gate", "w_up", "w_down")
F32, BF16 = jnp.float32, jnp.bfloat16
NN = (((1,), (0,)), ((), ()))
NT = (((1,), (1,)), ((), ()))


def dot(a, b, dims=NN):
    return lax.dot_general(a, b, dims, preferred_element_type=F32)


def normed(h):
    wide = h.astype(F32)
    scale = lax.rsqrt(jnp.mean(wide * wide, -1, keepdims=True) + 1e-6)
    return wide, scale


def sigmoid(g):
    return 0.5 * jnp.tanh(0.5 * g) + 0.5


def first_forward(x_ref, wg_ref, wu_ref, wd_ref, h_ref, g_ref, u_ref, hid_ref, *, cut):
    wide, scale = normed(x_ref[...])
    a = (wide * scale).astype(BF16)
    ff = wg_ref.shape[1]
    for j in range(0, ff, cut):
        g = dot(a, wg_ref[:, j : j + cut])
        u = dot(a, wu_ref[:, j : j + cut])
        g_ref[:, j : j + cut] = g
        u_ref[:, j : j + cut] = u
        hid_ref[:, j : j + cut] = (g * sigmoid(g) * u).astype(BF16)
    y = dot(hid_ref[...], wd_ref[...]).astype(BF16)
    h_ref[...] = x_ref[...] + y


def back_through(dh, wide, scale, da):
    inner = jnp.mean(da * wide, -1, keepdims=True)
    by_norm = scale * da - wide * (scale * scale * scale * inner)
    return dh + by_norm.astype(BF16)


def last_layer(h_ref, dy_ref, wg_ref, wu_ref, wd_ref, dh_ref, og_ref, ou_ref, od_ref, acc_g, acc_u, acc_d, dg_ref, du_ref, *, cut):
    i, n = pl.program_id(0), pl.num_programs(0)

    @pl.when(i == 0)
    def _():
        acc_g[...] = jnp.zeros_like(acc_g)
        acc_u[...] = jnp.zeros_like(acc_u)
        acc_d[...] = jnp.zeros_like(acc_d)

    wide, scale = normed(h_ref[...])
    a = (wide * scale).astype(BF16)
    dy = dy_ref[...]
    a_t, dy_t = a.T, dy.T
    ff = wg_ref.shape[1]
    for j in range(0, ff, cut):
        at = slice(j, j + cut)
        g = dot(a, wg_ref[:, at])
        u = dot(a, wu_ref[:, at])
        dhid = dot(dy, wd_ref[at, :], NT).astype(BF16).astype(F32)
        sig = sigmoid(g)
        s = g * sig
        hid = (s * u).astype(BF16)
        du = (dhid * s).astype(BF16)
        dg = (dhid * u * (sig * (1.0 + g - s))).astype(BF16)
        dg_ref[:, at] = dg
        du_ref[:, at] = du
        acc_d[:, at] += dot(dy_t, hid)
        acc_g[:, at] += dot(a_t, dg)
        acc_u[:, at] += dot(a_t, du)
    da = (dot(dg_ref[...], wg_ref[...], NT) + dot(du_ref[...], wu_ref[...], NT)).astype(BF16).astype(F32)
    dh_ref[...] = back_through(dy, wide, scale, da)

    @pl.when(i == n - 1)
    def _():
        og_ref[...] = acc_g[...].astype(BF16)
        ou_ref[...] = acc_u[...].astype(BF16)
        od_ref[...] = acc_d[...].T.astype(BF16)


def first_back(x_ref, dh_ref, g_ref, u_ref, wd_ref, og_ref, ou_ref, od_ref, acc_g, acc_u, acc_d, *, cut):
    i, n = pl.program_id(0), pl.num_programs(0)

    @pl.when(i == 0)
    def _():
        acc_g[...] = jnp.zeros_like(acc_g)
        acc_u[...] = jnp.zeros_like(acc_u)
        acc_d[...] = jnp.zeros_like(acc_d)

    wide, scale = normed(x_ref[...])
    a_t = (wide * scale).astype(BF16).T
    dh = dh_ref[...]
    dh_t = dh.T
    ff = g_ref.shape[1]
    for j in range(0, ff, cut):
        at = slice(j, j + cut)
        g, u = g_ref[:, at], u_ref[:, at]
        dhid = dot(dh, wd_ref[at, :], NT).astype(BF16).astype(F32)
        sig = sigmoid(g)
        s = g * sig
        hid = (s * u).astype(BF16)
        du = (dhid * s).astype(BF16)
        dg = (dhid * u * (sig * (1.0 + g - s))).astype(BF16)
        acc_d[:, at] += dot(dh_t, hid)
        acc_g[:, at] += dot(a_t, dg)
        acc_u[:, at] += dot(a_t, du)

    @pl.when(i == n - 1)
    def _():
        og_ref[...] = acc_g[...].astype(BF16)
        ou_ref[...] = acc_u[...].astype(BF16)
        od_ref[...] = acc_d[...].T.astype(BF16)


def whole(shape):
    return pl.BlockSpec(shape, lambda i: (0,) * len(shape), pipeline_mode=pl.Buffered(1))


def rows(n, width):
    return pl.BlockSpec((n, width), lambda i: (i, 0))


def struct(shape, dtype):
    return jax.ShapeDtypeStruct(shape, dtype)


def adamw(w, m, v, g):
    m = 0.9 * m + 0.1 * g
    v = 0.95 * v + 0.05 * g * g
    step = m * lax.rsqrt(v + 1e-8) + 0.1 * w
    return (w - 0.02 * step).astype(BF16), m, v


def solution(mesh):
    def fetched(weights, number):
        return [lax.all_gather(w[number], "s", axis=0, tiled=True) for w in weights]

    def summed(term):
        return lax.psum(lax.psum_scatter(term, "s", scatter_dimension=0, tiled=True), "r")

    def step(x, dy, *arrays):
        weights, m, v = (arrays[i : i + 3] for i in (0, 3, 6))
        x, dy = x[0], dy[0]
        tokens, d = x.shape
        ff = weights[0].shape[2]
        cut, tile = 256, 512
        params = pltpu.CompilerParams(vmem_limit_bytes=62 * 2**20, dimension_semantics=("arbitrary",))
        one = 2 * tokens * d * ff
        by0, by1 = fetched(weights, 0), fetched(weights, 1)
        h, g, u = pl.pallas_call(
            functools.partial(first_forward, cut=cut),
            grid=(tokens // tile,),
            in_specs=[rows(tile, d), whole((d, ff)), whole((d, ff)), whole((ff, d))],
            out_specs=[rows(tile, d), rows(tile, ff), rows(tile, ff)],
            out_shape=[struct((tokens, d), BF16), struct((tokens, ff), F32), struct((tokens, ff), F32)],
            scratch_shapes=[pltpu.VMEM((tile, ff), BF16)],
            compiler_params=params,
            cost_estimate=pl.CostEstimate(flops=3 * one, bytes_accessed=8 * tokens * ff, transcendentals=0),
            name="first_forward",
        )(x, *by0)
        grads = [struct((d, ff), BF16), struct((d, ff), BF16), struct((ff, d), BF16)]
        grad_specs = [whole((d, ff)), whole((d, ff)), whole((ff, d))]
        accs = [pltpu.VMEM((d, ff), F32)] * 3
        dh, *by_w1 = pl.pallas_call(
            functools.partial(last_layer, cut=cut),
            grid=(tokens // tile,),
            in_specs=[rows(tile, d), rows(tile, d), whole((d, ff)), whole((d, ff)), whole((ff, d))],
            out_specs=[rows(tile, d)] + grad_specs,
            out_shape=[struct((tokens, d), BF16)] + grads,
            scratch_shapes=accs + [pltpu.VMEM((tile, ff), BF16)] * 2,
            compiler_params=params,
            cost_estimate=pl.CostEstimate(flops=8 * one, bytes_accessed=8 * tokens * d, transcendentals=0),
            name="last_layer",
        )(h, dy, *by1)
        by_w0 = pl.pallas_call(
            functools.partial(first_back, cut=cut),
            grid=(tokens // tile,),
            in_specs=[rows(tile, d), rows(tile, d), rows(tile, ff), rows(tile, ff), whole((ff, d))],
            out_specs=grad_specs,
            out_shape=grads,
            scratch_shapes=accs,
            compiler_params=params,
            cost_estimate=pl.CostEstimate(flops=4 * one, bytes_accessed=8 * tokens * ff, transcendentals=0),
            name="first_back",
        )(x, dh, g, u, by0[2])
        mine = [[summed(t) for t in by_w] for by_w in (by_w0, by_w1)]
        gradients = [jnp.stack([a, b]).astype(F32) for a, b in zip(*mine)]
        new = [adamw(w.astype(F32), mm, vv, gg) for w, mm, vv, gg in zip(weights, m, v, gradients, strict=True)]
        return tuple(one[which] for which in range(3) for one in new)

    states, cut = P(("rep", "r", "s"), None, None), P(None, "s", None)
    return jax.shard_map(
        step,
        mesh=mesh,
        in_specs=(states, states) + (cut,) * 9,
        out_specs=(P("rep", "s", None),) * 9,
        check_vma=False,
    )
```

```python
import functools

import jax
import jax.numpy as jnp
from jax import lax
from jax.experimental import pallas as pl
from jax.experimental.pallas import tpu as pltpu
from jax.sharding import PartitionSpec as P

F32, BF16 = jnp.float32, jnp.bfloat16
NN = (((1,), (0,)), ((), ()))
NT = (((1,), (1,)), ((), ()))
ANY = pl.BlockSpec(memory_space=pl.ANY)
DMA = pltpu.SemaphoreType.DMA


def dot(a, b, dims=NN):
    return lax.dot_general(a, b, dims, preferred_element_type=F32)


def sigmoid(g):
    return 0.5 * jnp.tanh(0.5 * g) + 0.5


def normed(h):
    wide = h.astype(F32)
    scale = lax.rsqrt(jnp.mean(wide * wide, -1, keepdims=True) + 1e-6)
    return wide, scale


class Place:
    def __init__(self):
        s, z = lax.axis_index("s"), lax.axis_index("r")
        self.s, self.z, self.core, self.chip = s, z, s % 2, s // 2
        self.partner = s + 1 - 2 * self.core
        x, y = self.chip // 2, self.chip % 2
        self.chips = [2 * (x + (1 - 2 * x) * (j // 2)) + (y + (1 - 2 * y) * (j % 2)) for j in range(4)]
        self.peers = [2 * chip + self.core for chip in self.chips]
        self.z_pair = z + 1 - 2 * (z % 2)
        self.inner = (z + 1) // 2 % 2
        self.z_middle = 3 - z

    def barrier(self):
        sem = pltpu.get_barrier_semaphore()
        others = [{"s": self.partner}] + [{"s": p} for p in self.peers[1:]] + [{"r": (self.z + k) % 4} for k in (1, 2, 3)]
        for device in others:
            pl.semaphore_signal(sem, inc=1, device_id=device, device_id_type=pl.DeviceIdType.MESH)
        pl.semaphore_wait(sem, len(others))


def push(src, dst, send, recv, device):
    return pltpu.make_async_remote_copy(
        src_ref=src, dst_ref=dst, send_sem=send, recv_sem=recv, device_id=device, device_id_type=pl.DeviceIdType.MESH
    )


def gather_scratch(n):
    return [DMA((n,))] + [DMA((n, 2))] + [DMA((n, 3, 2))] * 4


class Gather:
    def __init__(self, place, shards, fulls, halved, sems):
        self.p, self.shards, self.fulls, self.halved = place, shards, fulls, halved
        self.own, self.pair, self.ici, self.core, self.along, self.core2 = sems
        self.h = place.z % 2

    def part(self, m, s, h):
        ref, rows = self.fulls[m], self.shards[m].shape[0]
        if not self.halved[m]:
            return ref.at[pl.ds(pl.multiple_of(s * rows, 16), rows)]
        if rows % 32 == 0:
            return ref.at[pl.ds(pl.multiple_of(s * rows + h * (rows // 2), 16), rows // 2)]
        c = ref.shape[1] // 2
        return ref.at[pl.ds(pl.multiple_of(s * rows, 16), rows), pl.ds(pl.multiple_of(h * c, 128), c)]

    def mine(self, m):
        ref, rows, h = self.shards[m], self.shards[m].shape[0], self.h
        if not self.halved[m]:
            return ref
        if rows % 32 == 0:
            return ref.at[pl.ds(pl.multiple_of(h * (rows // 2), 16), rows // 2)]
        c = ref.shape[1] // 2
        return ref.at[:, pl.ds(pl.multiple_of(h * c, 128), c)]

    def local(self, m):
        rows = self.shards[m].shape[0]
        return pltpu.make_async_copy(self.shards[m], self.fulls[m].at[pl.ds(pl.multiple_of(self.p.s * rows, 16), rows)], self.own.at[m])

    def own_rows(self, m, s):
        rows = self.shards[m].shape[0]
        here = self.fulls[m].at[pl.ds(pl.multiple_of(s * rows, 16), rows)]
        return push(self.shards[m], here, self.pair.at[m, 0], self.pair.at[m, 1], {"s": self.p.partner})

    def over_ici(self, m, j, s):
        return push(self.mine(m), self.part(m, s, self.h), self.ici.at[m, j - 1, 0], self.ici.at[m, j - 1, 1], {"s": self.p.peers[j]})

    def to_core(self, m, j, s):
        here = self.part(m, s, self.h)
        return push(here, here, self.core.at[m, j - 1, 0], self.core.at[m, j - 1, 1], {"s": self.p.partner})

    def along_z(self, m, j, h):
        here = self.part(m, self.p.peers[j], h)
        return push(here, here, self.along.at[m, j - 1, 0], self.along.at[m, j - 1, 1], {"r": self.p.z_pair})

    def to_core2(self, m, j, s):
        here = self.part(m, s, 1 - self.h)
        return push(here, here, self.core2.at[m, j - 1, 0], self.core2.at[m, j - 1, 1], {"s": self.p.partner})

    def other(self, j):
        return 2 * self.p.chips[j] + 1 - self.p.core

    def start(self, m):
        for j in (1, 2, 3):
            self.over_ici(m, j, self.p.s).start()
        self.local(m).start()
        self.own_rows(m, self.p.s).start()

    def relay(self, m):
        for j in (1, 2, 3):
            self.over_ici(m, j, self.p.peers[j]).wait_recv()
            if self.halved[m]:
                self.along_z(m, j, self.h).start()
            self.to_core(m, j, self.p.peers[j]).start()

    def relay2(self, m):
        if self.halved[m]:
            for j in (1, 2, 3):
                self.along_z(m, j, 1 - self.h).wait_recv()
                self.to_core2(m, j, self.p.peers[j]).start()

    def finish(self, m):
        self.local(m).wait()
        self.own_rows(m, self.p.partner).wait_recv()
        self.own_rows(m, self.p.s).wait_send()
        for j in (1, 2, 3):
            self.over_ici(m, j, self.p.s).wait_send()
            self.to_core(m, j, self.other(j)).wait_recv()
            self.to_core(m, j, self.p.peers[j]).wait_send()
            if self.halved[m]:
                self.along_z(m, j, self.h).wait_send()
                self.to_core2(m, j, self.other(j)).wait_recv()
                self.to_core2(m, j, self.p.peers[j]).wait_send()


def gather_kernel(*refs, halved):
    n = len(halved)
    shards, fulls, sems = refs[:n], refs[n : 2 * n], refs[2 * n :]
    place = Place()
    place.barrier()
    g = Gather(place, [s.at[0] for s in shards], fulls, halved, sems)
    for stage in (g.start, g.relay, g.relay2, g.finish):
        for m in range(n):
            stage(m)


def reduce_scratch(n, r, c):
    return [
        pltpu.VMEM((n, 4, r, c), BF16),
        pltpu.VMEM((n, 3, r, c), BF16),
        pltpu.VMEM((n, r, c), F32),
        pltpu.VMEM((n, 3, r, c), BF16),
        pltpu.VMEM((n, 2, r, c), BF16),
        pltpu.VMEM((n, 2, r, c), BF16),
        pltpu.VMEM((n, r, c), BF16),
        DMA((n, 2)),
        DMA((n, 3, 2)),
        DMA((n, 3, 2)),
    ]


class Reduce:
    def __init__(self, place, source, own, out, scratch, own_sem=None):
        self.p, self.source, self.own, self.out, self.own_sem = place, source, own, out, own_sem
        self.pair, self.sums, self.kept, self.got, self.sent_z, self.got_z, self.whole, self.s0, self.s1, self.s2 = scratch

    def swap(self, k):
        return push(self.source.at[k, :, 1 - self.p.core], self.pair.at[k], self.s0.at[k, 0], self.s0.at[k, 1], {"s": self.p.partner})

    def load(self, k):
        return pltpu.make_async_copy(self.source.at[k, :, self.p.core], self.own.at[k], self.own_sem.at[k])

    def spread(self, k, j):
        return push(self.sums.at[k, j - 1], self.got.at[k, j - 1], self.s1.at[k, j - 1, 0], self.s1.at[k, j - 1, 1], {"s": self.p.peers[j]})

    def inward(self, k):
        return push(self.sent_z.at[k, 0], self.got_z.at[k, 0], self.s2.at[k, 0, 0], self.s2.at[k, 0, 1], {"r": self.p.z_pair})

    def across(self, k):
        return push(self.sent_z.at[k, 1], self.got_z.at[k, 1], self.s2.at[k, 1, 0], self.s2.at[k, 1, 1], {"r": self.p.z_middle})

    def outward(self, k):
        return push(self.whole.at[k], self.whole.at[k], self.s2.at[k, 2, 0], self.s2.at[k, 2, 1], {"r": self.p.z_pair})

    def at_end(self, f):
        pl.when(self.p.inner == 0)(f)

    def in_middle(self, f):
        pl.when(self.p.inner == 1)(f)

    def stage(self, number, k):
        [self.stage0, self.stage1, self.stage2, self.stage3, self.stage4, self.stage5][number](k)

    def stage0(self, k):
        self.swap(k).start()
        if self.own_sem is not None:
            self.load(k).start()

    def stage1(self, k):
        if self.own_sem is not None:
            self.load(k).wait()
        self.swap(k).wait_recv()
        for j in (3, 1, 2, 0):
            chip = self.p.chips[j]
            mine = self.own[k, chip] if self.own_sem is not None else self.source[k, chip, self.p.core]
            total = mine.astype(F32) + self.pair[k, chip].astype(F32)
            if j:
                self.sums[k, j - 1] = total.astype(BF16)
                self.spread(k, j).start()
            else:
                self.kept[k] = total
        self.swap(k).wait_send()

    def stage2(self, k):
        for j in (1, 2, 3):
            self.spread(k, j).wait()
        total = self.kept[k]
        for j in range(3):
            total = total + self.got[k, j].astype(F32)
        self.kept[k] = total

        @self.at_end
        def _():
            self.sent_z[k, 0] = self.kept[k].astype(BF16)
            self.inward(k).start()

    def stage3(self, k):
        @self.in_middle
        def _():
            self.inward(k).wait_recv()
            self.sent_z[k, 1] = (self.kept[k] + self.got_z[k, 0].astype(F32)).astype(BF16)
            self.across(k).start()

    def stage4(self, k):
        @self.in_middle
        def _():
            self.across(k).wait()
            self.whole[k] = (self.sent_z[k, 1].astype(F32) + self.got_z[k, 1].astype(F32)).astype(BF16)
            self.outward(k).start()

    def stage5(self, k):
        @self.in_middle
        def _():
            self.outward(k).wait_send()

        @self.at_end
        def _():
            self.inward(k).wait_send()
            self.outward(k).wait_recv()

        self.out[k] = self.whole[k]

    def ticks(self, step, offsets, n):
        for t in (1, 5, 4, 3, 2):
            k = step - offsets[t]

            @pl.when((k >= 0) & (k < n))
            def _(k=k, t=t):
                self.stage(t, jnp.clip(k, 0, n - 1))


def first_forward(x_ref, wg_ref, wu_ref, wd_ref, *refs, cut, halved):
    n = len(halved)
    shards, refs = refs[:n], refs[n:]
    h_ref, g_ref, u_ref, at_ref = refs[:4]
    fulls, hid_ref, sems = refs[4 : 4 + n], refs[4 + n], refs[5 + n :]
    i = pl.program_id(0)
    place = Place()
    gather = Gather(place, [s.at[1] for s in shards], fulls, halved, sems)

    @pl.when(i == 0)
    def _():
        place.barrier()
        for m in range(n):
            gather.start(m)

    for m in range(n):
        pl.when(i == 2 + m)(functools.partial(gather.relay, m))
        pl.when(i == 4 + m + m // 2)(functools.partial(gather.relay2, m))

    wide, scale = normed(x_ref[...])
    a = (wide * scale).astype(BF16)
    at_ref[...] = a.T
    ff = wg_ref.shape[1]
    for j in range(0, ff, cut):
        g = dot(a, wg_ref[:, j : j + cut])
        u = dot(a, wu_ref[:, j : j + cut])
        g_ref[:, j : j + cut] = g
        u_ref[:, j : j + cut] = u
        hid_ref[:, j : j + cut] = (g * sigmoid(g) * u).astype(BF16)
    h_ref[...] = x_ref[...] + dot(hid_ref[...], wd_ref[...]).astype(BF16)

    @pl.when(i == pl.num_programs(0) - 1)
    def _():
        for m in range(n):
            gather.finish(m)


def swiglu_back(g, u, dhid):
    dhid = dhid.astype(BF16).astype(F32)
    sig = sigmoid(g)
    s = g * sig
    return (s * u).astype(BF16), (dhid * u * (sig * (1.0 + g - s))).astype(BF16), (dhid * s).astype(BF16)


def last_layer(h_ref, dy_ref, wg_ref, wu_ref, wd_ref, dh_ref, at_ref, dg_ref, du_ref, od_ref, acc_d, *, cut):
    i, n = pl.program_id(0), pl.num_programs(0)

    @pl.when(i == 0)
    def _():
        acc_d[...] = jnp.zeros_like(acc_d)

    wide, scale = normed(h_ref[...])
    a = (wide * scale).astype(BF16)
    at_ref[...] = a.T
    dy = dy_ref[...]
    dy_t = dy.T
    ff = wg_ref.shape[1]
    for j in range(0, ff, cut):
        at = slice(j, j + cut)
        g = dot(a, wg_ref[:, at])
        u = dot(a, wu_ref[:, at])
        hid, dg, du = swiglu_back(g, u, dot(dy, wd_ref[at, :], NT))
        dg_ref[:, at] = dg
        du_ref[:, at] = du
        acc_d[:, at] += dot(dy_t, hid)
    da = (dot(dg_ref[...], wg_ref[...], NT) + dot(du_ref[...], wu_ref[...], NT)).astype(BF16).astype(F32)
    inner = jnp.mean(da * wide, -1, keepdims=True)
    by_norm = scale * da - wide * (scale * scale * scale * inner)
    dh_ref[...] = dy + by_norm.astype(BF16)

    @pl.when(i == n - 1)
    def _():
        od_ref[...] = acc_d[...].T.astype(BF16)


def first_back(dh_ref, g_ref, u_ref, wd_ref, source, dg_ref, du_ref, od_ref, gu_ref, acc_d, own, own_sem, *scratch, cut, chunks):
    i, n = pl.program_id(0), pl.num_programs(0)
    place = Place()
    first, count = chunks
    reduce = Reduce(place, source.at[pl.ds(first, count)], own, gu_ref, scratch, own_sem)
    offsets = [0, 1, 3, 4, 5, 6]

    @pl.when(i == 0)
    def _():
        acc_d[...] = jnp.zeros_like(acc_d)
        place.barrier()
        for k in range(count):
            reduce.stage0(k)

    reduce.ticks(i, offsets, count)
    dh = dh_ref[...]
    dh_t = dh.T
    ff = g_ref.shape[1]
    for j in range(0, ff, cut):
        at = slice(j, j + cut)
        hid, dg, du = swiglu_back(g_ref[:, at], u_ref[:, at], dot(dh, wd_ref[at, :], NT))
        dg_ref[:, at] = dg
        du_ref[:, at] = du
        acc_d[:, at] += dot(dh_t, hid)

    @pl.when(i == n - 1)
    def _():
        od_ref[...] = acc_d[...].T.astype(BF16)

        @pl.loop(n, max(n, count + offsets[-1]))
        def _(step):
            reduce.ticks(step, offsets, count)


def by_weights(at_ref, dg_ref, du_ref, dsource, *refs, count, total):
    some = total > count
    if some:
        left_ref, refs = refs[0], refs[1:]
    gu_ref, d_ref, chunk, down_own, down_sem = refs[:5]
    i = pl.program_id(0)
    place = Place()
    down = Reduce(place, dsource, down_own, d_ref, refs[5:15], down_sem)
    gu = Reduce(place, chunk, None, gu_ref, refs[15:])
    down_offsets, gu_offsets = [0, 1, 5, 7, 8, 10], [0, 1, 5, 6, 7, 8]

    @pl.when(i == 0)
    def _():
        place.barrier()
        down.stage0(0)

    def ticks(step):
        down.ticks(step, down_offsets, 1)
        gu.ticks(step, gu_offsets, count)

    ticks(i)
    for half, ref in enumerate((dg_ref, du_ref)):
        block = dot(at_ref[...], ref[...]).astype(BF16)
        rows = block.shape[0] // 8
        for s in range(8):
            to = slice(half * rows, (half + 1) * rows)
            if some:
                left_ref[0, s // 2, s % 2, to] = block[s * rows : (s + 1) * rows]
            else:
                chunk[i, s // 2, s % 2, to] = block[s * rows : (s + 1) * rows]
    if some:

        @pl.when(i < count)
        def _():
            chunk[jnp.clip(i, 0, count - 1)] = left_ref[0]

    @pl.when(i < count)
    def _():
        gu.stage0(jnp.clip(i, 0, count - 1))

    @pl.when(i == total - 1)
    def _():
        @pl.loop(total, max(total, down_offsets[-1] + 1, count + gu_offsets[-1]))
        def _(step):
            ticks(step)


def whole(shape):
    return pl.BlockSpec(shape, lambda i: (0,) * len(shape), pipeline_mode=pl.Buffered(1))


def rows(n, width):
    return pl.BlockSpec((n, width), lambda i: (i, 0))


def columns(height, n):
    return pl.BlockSpec((height, n), lambda i: (0, i))


def struct(shape, dtype=BF16):
    return jax.ShapeDtypeStruct(shape, dtype)


def params(number=None, mib=62):
    extra = {} if number is None else {"collective_id": number, "has_side_effects": True}
    return pltpu.CompilerParams(vmem_limit_bytes=mib * 2**20, dimension_semantics=("arbitrary",), **extra)


def adamw(w, m, v, g):
    m = 0.9 * m + 0.1 * g
    v = 0.95 * v + 0.05 * g * g
    step = m * lax.rsqrt(v + 1e-8) + 0.1 * w
    return (w - 0.02 * step).astype(BF16), m, v


def solution(mesh):
    early = 2

    def step(x, dy, *arrays):
        weights, m, v = (arrays[i : i + 3] for i in (0, 3, 6))
        x, dy = x[0], dy[0]
        tokens, d = x.shape
        ff = weights[0].shape[2]
        cut, tile = 256, 512
        n, many = tokens // tile, ff // cut
        fulls = [struct((d, ff)), struct((d, ff)), struct((ff, d))]
        blocks = (d // 4, cut)
        down_blocks = (ff // 8, d)
        wide = struct((tokens, ff))

        by0 = pl.pallas_call(
            functools.partial(gather_kernel, halved=(True, True, False)),
            in_specs=[ANY] * 3,
            out_specs=[ANY] * 3,
            out_shape=fulls,
            scratch_shapes=gather_scratch(3),
            compiler_params=pltpu.CompilerParams(collective_id=0, has_side_effects=True),
            name="gather_first",
        )(*weights)

        h, g, u, a0_t, *by1 = pl.pallas_call(
            functools.partial(first_forward, cut=cut, halved=(True, True, True)),
            grid=(n,),
            in_specs=[rows(tile, d), whole((d, ff)), whole((d, ff)), whole((ff, d))] + [ANY] * 3,
            out_specs=[rows(tile, d), rows(tile, ff), rows(tile, ff), columns(d, tile)] + [ANY] * 3,
            out_shape=[struct((tokens, d)), struct((tokens, ff), F32), struct((tokens, ff), F32), struct((d, tokens))] + fulls,
            scratch_shapes=[pltpu.VMEM((tile, ff), BF16)] + gather_scratch(3),
            compiler_params=params(1),
            name="first_forward",
        )(x, *by0, *weights)

        dh, a1_t, dg1, du1, by_d1 = pl.pallas_call(
            functools.partial(last_layer, cut=cut),
            grid=(n,),
            in_specs=[rows(tile, d), rows(tile, d), whole((d, ff)), whole((d, ff)), whole((ff, d))],
            out_specs=[rows(tile, d), columns(d, tile), rows(tile, ff), rows(tile, ff), whole((ff, d))],
            out_shape=[struct((tokens, d)), struct((d, tokens)), wide, wide, struct((ff, d))],
            scratch_shapes=[pltpu.VMEM((d, ff), F32)],
            compiler_params=params(),
            name="last_layer",
        )(h, dy, *by1)

        def summed(a_t, dg, du, by_d, count, number):
            some = many > count
            outs = [struct((count,) + blocks), struct((1,) + down_blocks)]
            specs = [whole((count,) + blocks), whole((1,) + down_blocks)]
            if some:
                outs = [struct((many, 4, 2) + blocks)] + outs
                specs = [pl.BlockSpec((1, 4, 2) + blocks, lambda i: (i, 0, 0, 0, 0))] + specs
            return pl.pallas_call(
                functools.partial(by_weights, count=count, total=many),
                grid=(many,),
                in_specs=[whole((d, tokens)), columns(tokens, cut), columns(tokens, cut), ANY],
                out_specs=specs,
                out_shape=outs,
                scratch_shapes=[pltpu.VMEM((count, 4, 2) + blocks, BF16), pltpu.VMEM((1, 4) + down_blocks, BF16), DMA((1,))]
                + reduce_scratch(1, *down_blocks)
                + reduce_scratch(count, *blocks),
                compiler_params=params(number),
                name=f"by_weights_{number}",
            )(a_t, dg, du, by_d.reshape((1, 4, 2) + down_blocks))

        left, early_gu1, sum_d1 = summed(a1_t, dg1, du1, by_d1, early, 2)

        late = many - early
        dg0, du0, by_d0, late_gu1 = pl.pallas_call(
            functools.partial(first_back, cut=cut, chunks=(early, late)),
            grid=(n,),
            in_specs=[rows(tile, d), rows(tile, ff), rows(tile, ff), whole((ff, d)), ANY],
            out_specs=[rows(tile, ff), rows(tile, ff), whole((ff, d)), whole((late,) + blocks)],
            out_shape=[wide, wide, struct((ff, d)), struct((late,) + blocks)],
            scratch_shapes=[pltpu.VMEM((d, ff), F32), pltpu.VMEM((late, 4) + blocks, BF16), DMA((late,))] + reduce_scratch(late, *blocks),
            compiler_params=params(3),
            name="first_back",
        )(dh, g, u, by0[2], left)

        gu0, sum_d0 = summed(a0_t, dg0, du0, by_d0, many, 4)
        gu = jnp.stack([gu0, jnp.concatenate([early_gu1, late_gu1])])
        gu = gu.reshape(2, many, 2, d // 8, cut).transpose(2, 0, 3, 1, 4).reshape(2, 2, d // 8, ff)
        gradients = [gu[0], gu[1], jnp.concatenate([sum_d0, sum_d1])]
        new = [adamw(w.astype(F32), mm, vv, gg.astype(F32)) for w, mm, vv, gg in zip(weights, m, v, gradients, strict=True)]
        return tuple(one[which] for which in range(3) for one in new)

    states, cut = P(("rep", "r", "s"), None, None), P(None, "s", None)
    return jax.shard_map(
        step,
        mesh=mesh,
        in_specs=(states, states) + (cut,) * 9,
        out_specs=(P("rep", "s", None),) * 9,
        check_vma=False,
    )
```
